256 devices in a mesh: grp: 32 (over y, z), row: 8 (over x, core).
Axes of the slice: x: 4, y: 4, z: 8, core: 2. Of those that a mesh axis runs over, the one named last changes fastest.
Arguments:
- block: bfloat16 [65536, 1024], P(('grp', 'row')), may hold values from -6 to 6
- degree: int32 [65536], P(('grp', 'row')), may hold values from 1 to 3
- tile_values: bfloat16 [16384, 128, 128], P(('grp', 'row')), may hold values from -0.1875 to 0.1875
- tile_rows: int32 [16384], P(('grp', 'row')), may hold values from 0 to 1
- tile_cols: int32 [16384], P(('grp', 'row')), may hold values from 0 to 47
- tile_count: int32 [256], P(('grp', 'row')), may hold values from 24 to 64, as said below
- send_tiles: int32 [256, 32], P(('grp', 'row')), may hold values from 0 to 1
Outputs:
- logs: bfloat16 [65536, 1024], P(('grp', 'row'))
- gram: float32 [32768, 1024], P(('grp', 'row'))
The draws below stay inside these ranges and needn't reach their ends.
Inputs may be any that keep to these rules, and one draw needn't show every extreme that they name: Slots of a device at positions tile_count or later are padding; some device has all 64 slots live.
All inputs are finite; a program needn't handle non-finite values.
Results may differ from the reference program's by a relative error of at most 0.014.
Values may be sent and summed in bfloat16 or wider, within the bound.
No kernel may reach another device: no remote copies, remote signals or barrier semaphores. Data moves between devices by JAX's collectives and lax.ppermute only.
A program may use at most 128 MiB of HBM per device.

```python
import jax
import jax.numpy as jnp
from jax import lax

K = 1024
TILE = 128
ROWS_DEV = 256
SLOTS = 64
POWERS = 2
ROW_TILES = 2
NODES = 65536
SOURCES = 48
SLOTS_ALL = 16384
N_GRP = 32
N_ROW = 8


def draw_tile_count(key, part):
    first_key, second_key = jax.random.split(jax.random.fold_in(key, 7))
    devices = N_GRP * N_ROW
    drawn = jax.random.randint(first_key, (devices,), 0, SLOTS + 1)
    counts = jnp.minimum(SLOTS * 3 // 8 + drawn * drawn * 5 // (8 * SLOTS), SLOTS)
    chosen = jax.random.randint(second_key, (), 0, devices)
    counts = jnp.where(jnp.arange(devices) == chosen, SLOTS, counts)
    return counts.astype(jnp.int32)


def with_ends(values, stream_key, least, top_value):
    spot = [jax.random.randint(jax.random.fold_in(stream_key, axis), (), 0, length) for axis, length in enumerate(values.shape)]
    longest = values.shape.index(max(values.shape))
    beside = spot[:longest] + [(spot[longest] + 1) % values.shape[longest]] + spot[longest + 1:]
    return values.at[tuple(spot)].set(least).at[tuple(beside)].set(top_value)


def steps_of(key, extent, cuts, low, largest):
    gain, own = 1.0, jax.random.fold_in(key, 6)
    for axis_at, blocks in cuts:
        heights = jnp.exp(jax.random.uniform(jax.random.fold_in(own, axis_at), (blocks,), jnp.float32, low / len(cuts), largest / len(cuts)))
        gain = gain * jnp.repeat(heights, extent[axis_at] // blocks).reshape([-1 if axis == axis_at else 1 for axis in range(len(extent))])
    return gain


def centred(stream_key, extent, spread, reach, cuts=(), kind=jnp.bfloat16):
    gain = steps_of(stream_key, extent, cuts, -0.22, 0.18) if cuts else 1.0
    values = jax.random.normal(stream_key, extent, jnp.float32) * spread * gain
    return jnp.minimum(jnp.maximum(values, -reach), reach).astype(kind)


def setup_inputs(seed: int = 0) -> dict:
    key_of = jax.random.split(jax.random.key(seed), 8)
    return {
        "block": centred(key_of[0], (NODES, K), 1.0, 6.0, ((0, 256),)),
        "degree": with_ends(jax.random.randint(key_of[1], (NODES,), 1, 4), jax.random.fold_in(key_of[1], 1), 1, 3).astype(jnp.int32),
        "tile_values": centred(key_of[2], (SLOTS_ALL, TILE, TILE), (SLOTS * 16) ** -0.5, 0.1875, ((0, 256),)),
        "tile_rows": with_ends(jax.random.randint(key_of[3], (SLOTS_ALL,), 0, ROW_TILES), jax.random.fold_in(key_of[3], 1), 0, ROW_TILES - 1).astype(jnp.int32),
        "tile_cols": with_ends(jax.random.randint(key_of[4], (SLOTS_ALL,), 0, SOURCES), jax.random.fold_in(key_of[4], 1), 0, SOURCES - 1).astype(jnp.int32),
        "tile_count": draw_tile_count(jax.random.fold_in(key_of[7], 71), 0),
        "send_tiles": with_ends(jax.random.randint(key_of[6], (N_GRP * N_ROW, N_GRP), 0, ROW_TILES), jax.random.fold_in(key_of[6], 1), 0, ROW_TILES - 1).astype(jnp.int32),
    }


def column_tiles(tile_cols, send_tiles):
    row_tiles = ROWS_DEV // TILE
    slot_ids = jnp.arange(SLOTS * N_GRP * N_ROW, dtype=jnp.int32)
    device = slot_ids // SLOTS
    group = device // N_ROW
    member = device % N_ROW
    local_span = N_ROW * row_tiles
    source_group = jnp.maximum(tile_cols - local_span, 0)
    source_device = (source_group * N_ROW + member).astype(jnp.int32)
    remote = source_device * row_tiles + send_tiles[source_device, group]
    return jnp.where(tile_cols < local_span, group * local_span + tile_cols, remote).astype(jnp.int32)


def reference(block, degree, tile_values, tile_rows, tile_cols, tile_count, send_tiles):
    devices = N_GRP * N_ROW
    row_tiles = ROWS_DEV // TILE
    columns = column_tiles(tile_cols, send_tiles).reshape(devices, SLOTS)
    values = tile_values.reshape(devices, SLOTS, TILE, TILE)
    rows = tile_rows.reshape(devices, SLOTS)
    tile_ids = jnp.arange(row_tiles, dtype=jnp.int32)
    slot_pos = jnp.arange(SLOTS, dtype=jnp.int32)
    current = block
    power_sum = jnp.zeros(block.shape, jnp.float32)
    for power in range(POWERS):
        tiles_all = current.reshape(-1, TILE, K).astype(jnp.float32)

        def one_device(pieces):
            values_here, columns_here, rows_here, count_here = pieces
            picked = tiles_all[columns_here]
            products = jnp.einsum("sik,skf->sif", values_here.astype(jnp.float32), picked, precision=lax.Precision.HIGHEST)
            live_mask = slot_pos < count_here
            weights = ((rows_here[None, :] == tile_ids[:, None]) & live_mask[None, :]).astype(jnp.float32)
            return jnp.einsum("rs,sif->rif", weights, products, precision=lax.Precision.HIGHEST)

        summed = lax.map(one_device, (values, columns, rows, tile_count))
        current = (summed.reshape(-1, K) / degree[:, None].astype(jnp.float32)).astype(jnp.bfloat16)
        power_sum = power_sum + current.astype(jnp.float32)
    logs = jnp.log(jnp.maximum(3.0 * power_sum, 1.0)).astype(jnp.bfloat16)
    grouped = logs.reshape(N_GRP, N_ROW * ROWS_DEV, K)

    def group_gram(group_logs):
        return jnp.dot(group_logs.T, group_logs, preferred_element_type=jnp.float32)

    gram = lax.map(group_gram, grouped) / (N_ROW * ROWS_DEV)
    return logs, gram.reshape(N_GRP * K, K)
```

```python
import functools

import jax
import jax.numpy as jnp
from jax import lax
from jax.experimental import pallas as pl
from jax.experimental.pallas import tpu as pltpu
from jax.sharding import PartitionSpec as P


NY, NZ, NX, NC = 4, 8, 4, 2


def y_pairs(step):
    return [(y * NZ + z, (y + step) % NY * NZ + z) for y in range(NY) for z in range(NZ)]


def z_pairs(step):
    return [(y * NZ + z, y * NZ + (z + step) % NZ) for y in range(NY) for z in range(NZ)]


def x_pairs(step):
    return [(x * NC + c, (x + step) % NX * NC + c) for x in range(NX) for c in range(NC)]


def core_pairs():
    return [(x * NC + c, x * NC + 1 - c) for x in range(NX) for c in range(NC)]


def ring_y(value, step):
    return lax.ppermute(value, "grp", y_pairs(step))


def ring_z(value, step):
    return lax.ppermute(value, "grp", z_pairs(step))


def ring_x(value, step):
    return lax.ppermute(value, "row", x_pairs(step))


def swap_core(value):
    return lax.ppermute(value, "row", core_pairs())


def gather_y(lists):
    ahead = ring_y(lists, 1)
    behind = ring_y(lists, -1)
    far_low = ring_y(assemble([(ahead, 32, 0)], 32), 1)
    far_high = ring_y(assemble([(behind, 32, 0)], 32, 32), -1)
    return ahead, behind, far_low, far_high


def gather_z(rows, half):
    ahead = behind = rows
    from_ahead, from_behind = [], []
    for _ in range(1, 4):
        ahead = ring_z(ahead, 1)
        behind = ring_z(behind, -1)
        from_ahead.append(ahead)
        from_behind.append(behind)
    far_first = ring_z(ahead[:half], 1)
    far_second = ring_z(behind[half:], -1)
    return from_ahead, from_behind, (far_first, far_second)


def gather_x(rows, swaps):
    height = rows.shape[0]
    half = height // 2
    ahead = ring_x(rows, 1)
    behind = ring_x(rows, -1)
    far_first = ring_x(ahead[:half], 1)
    far_second = ring_x(behind[half:], -1)
    own, near = [(rows, height, 0)], [(ahead, height, 0), (behind, height, height)]
    far = [(far_first, half, 0), (far_second, half, half)]
    if swaps == 3:
        mine = [rows, assemble(near, 2 * height), assemble(far, height)]
    else:
        near = own + [(piece, size, place + height) for piece, size, place in near]
        mine = [assemble(near, 3 * height), assemble(far, height)]
    theirs = []
    for block in mine:
        theirs.append(swap_core(block))
    return mine + theirs


POSITIONS = (0, 1, 3, 2)
SOURCE_ROWS = 16 * 1024
LATE_RANKS = (3, 4, 5)
CHUNK = 8
SMEM = pl.BlockSpec(memory_space=pltpu.SMEM)
VMEM = pl.BlockSpec(memory_space=pltpu.VMEM)
ANY = pl.BlockSpec(memory_space=pl.ANY)
SMALL = pltpu.CompilerParams(vmem_limit_bytes=12 * 2**20)


def start_copies(pairs, sems, origin=0):
    copies = []
    for source, target, rows, place in pairs:
        copy = pltpu.make_async_copy(
            source.at[pl.ds(origin, rows)], target.at[pl.ds(place, rows)], sems.at[len(copies)]
        )
        copy.start()
        copies.append(copy)
    return copies


def assemble_body(spans, origin, *refs):
    pieces, out_ref, sems = refs[: len(spans)], refs[-2], refs[-1]
    for copy in start_copies([(piece, out_ref, *span) for piece, span in zip(pieces, spans)], sems, origin):
        copy.wait()


def assemble(parts, height, origin=0):
    pieces = [piece for piece, _, _ in parts]
    return pl.pallas_call(
        functools.partial(assemble_body, [(rows, place) for _, rows, place in parts], origin),
        in_specs=[ANY] * len(parts),
        out_specs=VMEM,
        out_shape=jax.ShapeDtypeStruct((height, *pieces[0].shape[1:]), pieces[0].dtype),
        scratch_shapes=[pltpu.SemaphoreType.DMA((len(parts),))],
        compiler_params=SMALL,
        cost_estimate=pl.CostEstimate(flops=300_000_000, bytes_accessed=2**22, transcendentals=0),
        name="assemble",
    )(*pieces)


def stack_body(*refs):
    pieces, out_ref, sems = refs[:3], refs[3], refs[4]
    copies = start_copies([(piece, out_ref, 256, 256 * k) for k, piece in enumerate(pieces)], sems)
    row_ids = lax.broadcasted_iota(jnp.int32, (16, 256), 0)
    notes = jnp.zeros((16, 256), jnp.float32)
    for k, piece in enumerate(pieces):
        line = piece[pl.ds(256, 16), :].astype(jnp.float32)[:1]
        notes = jnp.where(row_ids == k + 1, jnp.broadcast_to(line, (16, 256)), notes)
    out_ref[pl.ds(768, 16), :] = notes.astype(jnp.bfloat16)
    for copy in copies:
        copy.wait()


def stack(pieces):
    return pl.pallas_call(
        stack_body,
        in_specs=[VMEM] * 3,
        out_specs=VMEM,
        out_shape=jax.ShapeDtypeStruct((784, 256), jnp.bfloat16),
        scratch_shapes=[pltpu.SemaphoreType.DMA((3,))],
        compiler_params=SMALL,
        cost_estimate=pl.CostEstimate(flops=100_000_000, bytes_accessed=2**20, transcendentals=0),
        name="stack",
    )(*pieces)


def choices_body(ranks, *refs):
    out_ref = refs[-1]
    out_ref[...] = jnp.zeros_like(out_ref)
    row_ids = lax.broadcasted_iota(jnp.int32, (8, 128), 0)
    for k, rank in enumerate(ranks):
        own, rest = [ref[ref.shape[0] - 16 :, 128:256].astype(jnp.float32)[:8] for ref in refs[2 * k : 2 * k + 2]]
        out_ref[rank * 8 : rank * 8 + 8, :] = jnp.where(row_ids == 0, own, rest).astype(jnp.int32)


def choices(owns, rests):
    ranks = [rank for rank, holder in enumerate(owns) if holder is not None]
    holders = [holder for rank in ranks for holder in (owns[rank], rests[rank])]
    return pl.pallas_call(
        functools.partial(choices_body, ranks),
        in_specs=[VMEM] * len(holders),
        out_specs=VMEM,
        out_shape=jax.ShapeDtypeStruct((72, 128), jnp.int32),
        compiler_params=SMALL,
        cost_estimate=pl.CostEstimate(flops=100_000_000, bytes_accessed=2**16, transcendentals=0),
        name="choices",
    )(*holders)


LATE_FIRST = LATE_RANKS[0] * 1024


def power_body(plan, code_ref, bound_ref, table_ref, group_ref, degree_ref, *refs):
    groups, phase, last, spans = plan
    piece_refs, refs = refs[: len(spans)], refs[len(spans):]
    list_refs, refs = refs[: len(groups)], refs[len(groups):]
    x_ref = before_ref = sum_ref = None
    if phase != "late":
        x_ref, refs = refs[0], refs[1:]
    if phase == "late":
        sum_ref, refs = refs[0], refs[1:]
    if last and phase != "early":
        before_ref, refs = refs[0], refs[1:]
    out_ref, acc_ref, late_ref, sems = refs
    copies = start_copies([(piece, late_ref, *span) for piece, span in zip(piece_refs, spans)], sems)
    for copy in copies:
        copy.wait()

    def add_slots(member, list_ref, local, source_ref, origin, start, stop):
        group = group_ref[member]

        @pl.loop(0, (stop - start + CHUNK - 1) // CHUNK)
        def _(step):
            tops, lows, rights = [], [], []
            for k in range(CHUNK):
                place = start + step * CHUNK + k
                code = code_ref[member, jnp.minimum(place, 63)]
                live = place < stop
                row = (code >> 14) & 1
                source = ((code & 127) + table_ref[(code >> 7) & 127, group]) * 128 - origin
                source = pl.multiple_of(jnp.where(live, source, 0), 128)
                tile = list_ref[local * 64 + (code >> 15)]
                zero = jnp.zeros_like(tile)
                tops.append(jnp.where(live & (row == 0), tile, zero))
                lows.append(jnp.where(live & (row == 1), tile, zero))
                rights.append(source_ref[pl.ds(source, 128), :])
            left = jnp.concatenate([jnp.concatenate(tops, axis=1), jnp.concatenate(lows, axis=1)], axis=0)
            right = jnp.concatenate(rights, axis=0)
            acc_ref[...] += jnp.dot(left, right, preferred_element_type=jnp.float32)

    done = 0
    for (first, count), list_ref in zip(groups, list_refs):

        @pl.loop(0, count)
        def _(local, first=first, list_ref=list_ref, done=done):
            member = first + local
            base = (done + local) * 256
            here = pl.ds(pl.multiple_of(base, 256), 256)
            acc_ref[...] = sum_ref[here, :] if phase == "late" else jnp.zeros_like(acc_ref)
            middle, end = bound_ref[0, member], bound_ref[1, member]
            if phase != "late":
                add_slots(member, list_ref, local, x_ref, 0, 0, middle)
            if phase != "early":
                add_slots(member, list_ref, local, late_ref, LATE_FIRST, middle, end)
            else:
                out_ref[here, :] = acc_ref[...]
                return
            for half in range(2):
                place = pl.ds(pl.multiple_of(base + half * 128, 128), 128)
                scale = jnp.broadcast_to(degree_ref[member][:1, half * 128 : half * 128 + 128], (128, 128)).T
                scale = jnp.concatenate([scale, scale], axis=1)
                value = (acc_ref[pl.ds(half * 128, 128), :] / scale).astype(jnp.bfloat16)
                if last:
                    total = before_ref[place, :].astype(jnp.float32) + value.astype(jnp.float32)
                    value = jnp.log(jnp.maximum(3.0 * total, 1.0)).astype(jnp.bfloat16)
                out_ref[place, :] = value

        done += count


def power(groups, phase, notes, lists, sources=None, late=(), sums=None, before=None, last=False):
    pieces = [piece for piece, _, _ in late]
    spans = [(rows, place - LATE_FIRST) for _, rows, place in late]
    extra = [value for value in (sources, sums, before) if value is not None]
    count = sum(count for _, count in groups)
    return pl.pallas_call(
        functools.partial(power_body, (groups, phase, last, spans)),
        in_specs=[SMEM] * 4 + [VMEM] + [ANY] * len(pieces) + [VMEM] * (len(lists) + len(extra)),
        out_specs=VMEM,
        out_shape=jax.ShapeDtypeStruct((count * 256, 256), jnp.float32 if phase == "early" else jnp.bfloat16),
        scratch_shapes=[
            pltpu.VMEM((256, 256), jnp.float32),
            pltpu.VMEM((len(LATE_RANKS) * 1024 if pieces else 16, 256), jnp.bfloat16),
            pltpu.SemaphoreType.DMA((max(len(pieces), 1),)),
        ],
        compiler_params=SMALL,
        cost_estimate=pl.CostEstimate(
            flops=count * 600_000_000, bytes_accessed=10 * 2**20, transcendentals=0
        ),
    )(*notes, *pieces, *lists, *extra)


def step_parts(ahead, behind, step, rows, offset):
    return [(ahead[step - 1], rows, step * 1024 + offset), (behind[step - 1], rows, (8 - step) * 1024 + offset)]


def x_parts(blocks):
    parts, place = [], 8192
    for block in blocks:
        parts.append((block, block.shape[0], place))
        place += block.shape[0]
    return parts


def far_parts(far, rows, offset):
    return [(far[0], rows, 4096 + offset), (far[1], rows, 4096 + offset + rows)]


def step_body(block, degree, tile_values, tile_rows, tile_cols, tile_count, send_tiles):
    bf16 = jnp.bfloat16
    i32 = jnp.int32
    group = lax.axis_index("grp")
    y, z = group // NZ, group % NZ
    rank = lax.axis_index("row")
    x, core = rank // NC, rank % NC
    extra = jnp.concatenate([tile_rows, tile_cols, send_tiles[0], tile_count, jnp.zeros((95,), i32), degree])
    extra = lax.optimization_barrier(extra.reshape(2, 256))
    extra = jnp.pad(extra, ((0, 14), (0, 0))).astype(bf16)
    pieces = []
    for step in POSITIONS:
        cut = lax.dynamic_slice_in_dim(block, (y + step) % NY * 256, 256, 1)
        cut = jnp.concatenate([cut, extra], axis=0)
        pieces.append(ring_y(cut, step) if step else cut)
    ahead_lists, behind_lists, far_low, far_high = gather_y(tile_values)
    own, rest = pieces[0], stack(pieces[1:])
    degrees = jnp.concatenate([piece[257:258] for piece in pieces], axis=0).astype(jnp.float32)
    degrees = jnp.broadcast_to(degrees[:, None, :], (NY, 8, 256))

    lines = jnp.arange(NY)[:, None]
    told = jnp.where(lines == 0, own[256:260], rest[768:772]).astype(i32)
    rows, cols, counts = told[:, :64], told[:, 64:128], told[:, 160]
    steps = jnp.array(POSITIONS, i32)
    groups = (y - steps) % NY * NZ + z
    distant = jnp.maximum(cols - 16, 0)
    apart = (y - distant // NZ) % NY
    z_rank = (z - distant % NZ) % NZ
    spot = z_rank * NY + jnp.where(apart == 2, 3, jnp.where(apart == 3, 2, apart))
    near = jnp.minimum(cols, 15)
    near_rank = near // 2
    away = (x - near_rank // NC) % NX
    flip = (core + near_rank) % NC
    away = jnp.where(away == 2, 3, jnp.where(away == 3, 2, away))
    near_place = 64 + (flip * 4 + away) * 8 + jnp.arange(NY, dtype=i32)[:, None] * 2 + near % 2
    is_near = cols < 16
    slots = jnp.arange(64, dtype=i32)[None]
    choice = z_rank * 8 + spot % NY
    code = jnp.where(is_near, near_place + 64 * 128, spot * 2 + choice * 128) + rows * 2**14 + slots * 2**15
    late = (~is_near) & (z_rank >= LATE_RANKS[0]) & (z_rank <= LATE_RANKS[-1])
    dead = slots >= counts[:, None]
    key = jnp.where(dead, 2, late.astype(i32)) * 64 + slots
    position = jnp.sum((key[:, None, :] < key[:, :, None]).astype(i32), axis=2)
    code = jnp.sum(jnp.where(position[:, None, :] == slots[0][None, :, None], code[:, None, :], 0), axis=2)
    bounds = jnp.stack([jnp.sum((key < 64).astype(i32), axis=1), jnp.minimum(counts, 64)])

    own_z = gather_z(own, 128)
    rest_z = gather_z(rest, 384)
    first = assemble([(own, 256, 0), (rest, 768, 256)], 1024)
    base = x_parts(gather_x(first, 2))

    def z_steps(step, *rings):
        return [part for (ahead, behind, _), rows, offset in rings for part in step_parts(ahead, behind, step, rows, offset)]

    rings = (own_z, 256, 0), (rest_z, 768, 256)
    known = z_steps(1, *rings) + z_steps(2, *rings)
    sources = assemble([(first, 1024, 0), *known, *base], SOURCE_ROWS)
    lists = [assemble([(tile_values, 64, 0), (ahead_lists, 64, 64), (behind_lists, 64, 128)], 192)]
    lists.append(assemble([(far_low, 32, 0), (far_high, 32, 32)], 64))

    def by_rank(mine, ring):
        ahead, behind, far = ring
        return [mine, *ahead, far[1], *behind[::-1]]

    owns, rests = by_rank(own, own_z), by_rank(rest, rest_z)
    early_ranks = [None if rank in LATE_RANKS else holder for rank, holder in enumerate(owns)]
    table = choices(early_ranks, rests)
    sums = power([(0, 3)], "early", [code, bounds, table, groups, degrees], lists[:1], sources)
    notes = [code, bounds, choices(owns, rests), groups, degrees]
    late = z_steps(3, *rings) + far_parts(own_z[2], 128, 0) + far_parts(rest_z[2], 384, 256)
    most = power([(0, 3)], "late", notes, lists[:1], None, late, sums)
    most_z = gather_z(most, 384)
    few = power([(3, 1)], "all", notes, lists[1:], sources, late)
    few_z = gather_z(few, 128)
    second = assemble([(most, 768, 0), (few, 256, 768)], 1024)
    base = x_parts(gather_x(second, 2))
    rings = (most_z, 768, 0), (few_z, 256, 768)
    known = z_steps(1, *rings) + z_steps(2, *rings)
    sources = assemble([(second, 1024, 0), *known, *base], SOURCE_ROWS)
    sums = power([(0, 3), (3, 1)], "early", notes, lists, sources, last=True)
    late = z_steps(3, *rings) + far_parts(most_z[2], 384, 0) + far_parts(few_z[2], 128, 768)
    logs_cut = power([(0, 3), (3, 1)], "late", notes, lists, None, late, sums, second, True)
    logs = jnp.zeros((256, 1024), bf16)
    for place, step in enumerate(POSITIONS):
        piece = logs_cut[place * 256 : place * 256 + 256]
        piece = ring_y(piece, -step) if step else piece
        logs = lax.dynamic_update_slice_in_dim(logs, piece, (y + step) % NY * 256, 1)
    contract = (((0,), (0,)), ((), ()))
    gram = jnp.zeros((128, 1024), jnp.float32)
    for rows in gather_x(logs, 3):
        columns = lax.dynamic_slice_in_dim(rows, rank * 128, 128, 1)
        gram += lax.dot_general(columns, rows, contract, preferred_element_type=jnp.float32)
    return logs, gram / 2048


def solution(mesh):
    placed = (
        P(("grp", "row"), None),
        P(("grp", "row")),
        P(("grp", "row"), None, None),
        P(("grp", "row")),
        P(("grp", "row")),
        P(("grp", "row")),
        P(("grp", "row"), None),
    )

    return jax.shard_map(
        step_body,
        mesh=mesh,
        in_specs=placed,
        out_specs=(P(("grp", "row"), None), P(("grp", "row"), None)),
        check_vma=False,
    )
```

```python
import functools

import jax
import jax.numpy as jnp
from jax import lax
from jax.experimental import pallas as pl
from jax.experimental.pallas import tpu as pltpu
from jax.sharding import PartitionSpec as P


NY, NZ, NX, NC = 4, 8, 4, 2


def y_pairs(step):
    return [(y * NZ + z, (y + step) % NY * NZ + z) for y in range(NY) for z in range(NZ)]


def z_pairs(step):
    return [(y * NZ + z, y * NZ + (z + step) % NZ) for y in range(NY) for z in range(NZ)]


def x_pairs(step):
    return [(x * NC + c, (x + step) % NX * NC + c) for x in range(NX) for c in range(NC)]


def core_pairs():
    return [(x * NC + c, x * NC + 1 - c) for x in range(NX) for c in range(NC)]


def ring_y(value, step):
    return lax.ppermute(value, "grp", y_pairs(step))


def ring_z(value, step):
    return lax.ppermute(value, "grp", z_pairs(step))


def ring_x(value, step):
    return lax.ppermute(value, "row", x_pairs(step))


def swap_core(value):
    return lax.ppermute(value, "row", core_pairs())


def gather_y(lists):
    ahead = ring_y(lists, 1)
    behind = ring_y(lists, -1)
    far_low = ring_y(assemble([(ahead, 32, 0)], 32), 1)
    far_high = ring_y(assemble([(behind, 32, 0)], 32, 32), -1)
    return ahead, behind, far_low, far_high


def gather_z(rows, half):
    ahead = behind = rows
    from_ahead, from_behind = [], []
    for _ in range(1, 4):
        ahead = ring_z(ahead, 1)
        behind = ring_z(behind, -1)
        from_ahead.append(ahead)
        from_behind.append(behind)
    far_first = ring_z(ahead[:half], 1)
    far_second = ring_z(behind[half:], -1)
    return from_ahead, from_behind, (far_first, far_second)


def gather_x(rows, swaps):
    height = rows.shape[0]
    half = height // 2
    ahead = ring_x(rows, 1)
    behind = ring_x(rows, -1)
    far_first = ring_x(ahead[:half], 1)
    far_second = ring_x(behind[half:], -1)
    own, near = [(rows, height, 0)], [(ahead, height, 0), (behind, height, height)]
    far = [(far_first, half, 0), (far_second, half, half)]
    if swaps == 3:
        mine = [rows, assemble(near, 2 * height), assemble(far, height)]
    else:
        near = own + [(piece, size, place + height) for piece, size, place in near]
        mine = [assemble(near, 3 * height), assemble(far, height)]
    theirs = []
    for block in mine:
        theirs.append(swap_core(block))
    return mine + theirs


POSITIONS = (0, 1, 3, 2)
SOURCE_ROWS = 16 * 1024
LATE_RANKS = (3, 4, 5)
SMEM = pl.BlockSpec(memory_space=pltpu.SMEM)
VMEM = pl.BlockSpec(memory_space=pltpu.VMEM)
ANY = pl.BlockSpec(memory_space=pl.ANY)
SMALL = pltpu.CompilerParams(vmem_limit_bytes=12 * 2**20)


def start_copies(pairs, sems, origin=0):
    copies = []
    for source, target, rows, place in pairs:
        copy = pltpu.make_async_copy(
            source.at[pl.ds(origin, rows)], target.at[pl.ds(place, rows)], sems.at[len(copies)]
        )
        copy.start()
        copies.append(copy)
    return copies


def assemble_body(spans, origin, *refs):
    pieces, out_ref, sems = refs[: len(spans)], refs[-2], refs[-1]
    for copy in start_copies([(piece, out_ref, *span) for piece, span in zip(pieces, spans)], sems, origin):
        copy.wait()


def assemble(parts, height, origin=0):
    pieces = [piece for piece, _, _ in parts]
    return pl.pallas_call(
        functools.partial(assemble_body, [(rows, place) for _, rows, place in parts], origin),
        in_specs=[ANY] * len(parts),
        out_specs=VMEM,
        out_shape=jax.ShapeDtypeStruct((height, *pieces[0].shape[1:]), pieces[0].dtype),
        scratch_shapes=[pltpu.SemaphoreType.DMA((len(parts),))],
        compiler_params=SMALL,
        cost_estimate=pl.CostEstimate(flops=300_000_000, bytes_accessed=2**22, transcendentals=0),
        name="assemble",
    )(*pieces)


def stack_body(*refs):
    pieces, out_ref, sems = refs[:4], refs[4], refs[5]
    copies = start_copies([(piece, out_ref, 256, 256 * k) for k, piece in enumerate(pieces)], sems)
    row_ids = lax.broadcasted_iota(jnp.int32, (16, 256), 0)
    notes = jnp.zeros((16, 256), jnp.float32)
    for k, piece in enumerate(pieces):
        line = piece[pl.ds(256, 16), :].astype(jnp.float32)[:1]
        notes = jnp.where(row_ids == k, jnp.broadcast_to(line, (16, 256)), notes)
    out_ref[pl.ds(1024, 16), :] = notes.astype(jnp.bfloat16)
    for copy in copies:
        copy.wait()


def stack(pieces):
    return pl.pallas_call(
        stack_body,
        in_specs=[VMEM] * 4,
        out_specs=VMEM,
        out_shape=jax.ShapeDtypeStruct((1040, 256), jnp.bfloat16),
        scratch_shapes=[pltpu.SemaphoreType.DMA((4,))],
        compiler_params=SMALL,
        cost_estimate=pl.CostEstimate(flops=100_000_000, bytes_accessed=2**20, transcendentals=0),
        name="stack",
    )(*pieces)


def choices_body(ranks, *refs):
    out_ref = refs[-1]
    out_ref[...] = jnp.zeros_like(out_ref)
    for ref, rank in zip(refs, ranks):
        lines = ref[ref.shape[0] - 16 :, 128:256].astype(jnp.float32)[:8]
        out_ref[rank * 8 : rank * 8 + 8, :] = lines.astype(jnp.int32)


def choices(holders):
    ranks = [rank for rank, holder in enumerate(holders) if holder is not None]
    return pl.pallas_call(
        functools.partial(choices_body, ranks),
        in_specs=[VMEM] * len(ranks),
        out_specs=VMEM,
        out_shape=jax.ShapeDtypeStruct((72, 128), jnp.int32),
        compiler_params=SMALL,
        cost_estimate=pl.CostEstimate(flops=100_000_000, bytes_accessed=2**16, transcendentals=0),
        name="choices",
    )(*[holders[rank] for rank in ranks])


LATE_FIRST = LATE_RANKS[0] * 1024


def power_body(plan, code_ref, bound_ref, table_ref, group_ref, degree_ref, *refs):
    groups, phase, last, spans = plan
    piece_refs, refs = refs[: len(spans)], refs[len(spans):]
    list_refs, refs = refs[: len(groups)], refs[len(groups):]
    x_ref = before_ref = sum_ref = None
    if phase != "late":
        x_ref, refs = refs[0], refs[1:]
    if phase == "late":
        sum_ref, refs = refs[0], refs[1:]
    if last and phase != "early":
        before_ref, refs = refs[0], refs[1:]
    out_ref, acc_ref, late_ref, sems = refs
    copies = start_copies([(piece, late_ref, *span) for piece, span in zip(piece_refs, spans)], sems)
    for copy in copies:
        copy.wait()

    def add_slots(member, list_ref, local, source_ref, origin, row, start, stop, chunk):
        group = group_ref[member]
        half = pl.ds(row * 128, 128)

        @pl.loop(0, (stop - start + chunk - 1) // chunk)
        def _(step):
            lefts, rights = [], []
            for k in range(chunk):
                place = start + step * chunk + k
                code = code_ref[member, jnp.minimum(place, 63)]
                live = place < stop
                source = ((code & 127) + table_ref[(code >> 7) & 127, group]) * 128 - origin
                source = pl.multiple_of(jnp.where(live, source, 0), 128)
                tile = list_ref[local * 64 + (code >> 15)]
                lefts.append(jnp.where(live, tile, jnp.zeros_like(tile)))
                rights.append(source_ref[pl.ds(source, 128), :])
            left = jnp.concatenate(lefts, axis=1)
            right = jnp.concatenate(rights, axis=0)
            acc_ref[half, :] += jnp.dot(left, right, preferred_element_type=jnp.float32)

    done = 0
    for (first, count), list_ref in zip(groups, list_refs):

        @pl.loop(0, count)
        def _(local, first=first, list_ref=list_ref, done=done):
            member = first + local
            base = (done + local) * 256
            here = pl.ds(pl.multiple_of(base, 256), 256)
            acc_ref[...] = sum_ref[here, :] if phase == "late" else jnp.zeros_like(acc_ref)
            ends = [0] + [bound_ref[k, member] for k in range(4)]
            for row in range(2):
                if phase != "late":
                    add_slots(member, list_ref, local, x_ref, 0, row, ends[row], ends[row + 1], 16)
                if phase != "early":
                    add_slots(member, list_ref, local, late_ref, LATE_FIRST, row, ends[row + 2], ends[row + 3], 8)
            if phase == "early":
                out_ref[here, :] = acc_ref[...]
                return
            for half in range(2):
                place = pl.ds(pl.multiple_of(base + half * 128, 128), 128)
                scale = jnp.broadcast_to(degree_ref[member][:1, half * 128 : half * 128 + 128], (128, 128)).T
                scale = jnp.concatenate([scale, scale], axis=1)
                value = (acc_ref[pl.ds(half * 128, 128), :] / scale).astype(jnp.bfloat16)
                if last:
                    total = before_ref[place, :].astype(jnp.float32) + value.astype(jnp.float32)
                    value = jnp.log(jnp.maximum(3.0 * total, 1.0)).astype(jnp.bfloat16)
                out_ref[place, :] = value

        done += count


def power(groups, phase, notes, lists, sources=None, late=(), sums=None, before=None, last=False):
    pieces = [piece for piece, _, _ in late]
    spans = [(rows, place - LATE_FIRST) for _, rows, place in late]
    extra = [value for value in (sources, sums, before) if value is not None]
    count = sum(count for _, count in groups)
    return pl.pallas_call(
        functools.partial(power_body, (groups, phase, last, spans)),
        in_specs=[SMEM] * 4 + [VMEM] + [ANY] * len(pieces) + [VMEM] * (len(lists) + len(extra)),
        out_specs=VMEM,
        out_shape=jax.ShapeDtypeStruct((count * 256, 256), jnp.float32 if phase == "early" else jnp.bfloat16),
        scratch_shapes=[
            pltpu.VMEM((256, 256), jnp.float32),
            pltpu.VMEM((len(LATE_RANKS) * 1024 if pieces else 16, 256), jnp.bfloat16),
            pltpu.SemaphoreType.DMA((max(len(pieces), 1),)),
        ],
        compiler_params=SMALL,
        cost_estimate=pl.CostEstimate(
            flops=count * 600_000_000, bytes_accessed=10 * 2**20, transcendentals=0
        ),
    )(*notes, *pieces, *lists, *extra)


def step_parts(ahead, behind, step, rows, offset):
    return [(ahead[step - 1], rows, step * 1024 + offset), (behind[step - 1], rows, (8 - step) * 1024 + offset)]


def x_parts(blocks):
    parts, place = [], 8192
    for block in blocks:
        parts.append((block, block.shape[0], place))
        place += block.shape[0]
    return parts


def far_parts(far, rows, offset):
    return [(far[0], rows, 4096 + offset), (far[1], rows, 4096 + offset + rows)]


def step_body(block, degree, tile_values, tile_rows, tile_cols, tile_count, send_tiles):
    bf16 = jnp.bfloat16
    i32 = jnp.int32
    group = lax.axis_index("grp")
    y, z = group // NZ, group % NZ
    rank = lax.axis_index("row")
    x, core = rank // NC, rank % NC
    extra = jnp.concatenate([tile_rows, tile_cols, send_tiles[0], tile_count, jnp.zeros((95,), i32), degree])
    extra = lax.optimization_barrier(extra.reshape(2, 256))
    extra = jnp.pad(extra, ((0, 14), (0, 0))).astype(bf16)
    pieces = []
    for step in POSITIONS:
        cut = lax.dynamic_slice_in_dim(block, (y + step) % NY * 256, 256, 1)
        cut = jnp.concatenate([cut, extra], axis=0)
        pieces.append(ring_y(cut, step) if step else cut)
    ahead_lists, behind_lists, far_low, far_high = gather_y(tile_values)
    first = stack(pieces)
    degrees = jnp.concatenate([piece[257:258] for piece in pieces], axis=0).astype(jnp.float32)
    degrees = jnp.broadcast_to(degrees[:, None, :], (NY, 8, 256))

    told = first[1024:1040].astype(i32)[:NY]
    rows, cols, counts = told[:, :64], told[:, 64:128], told[:, 160]
    steps = jnp.array(POSITIONS, i32)
    groups = (y - steps) % NY * NZ + z
    distant = jnp.maximum(cols - 16, 0)
    apart = (y - distant // NZ) % NY
    z_rank = (z - distant % NZ) % NZ
    spot = z_rank * NY + jnp.where(apart == 2, 3, jnp.where(apart == 3, 2, apart))
    near = jnp.minimum(cols, 15)
    near_rank = near // 2
    away = (x - near_rank // NC) % NX
    flip = (core + near_rank) % NC
    away = jnp.where(away == 2, 3, jnp.where(away == 3, 2, away))
    near_place = 64 + (flip * 4 + away) * 8 + jnp.arange(NY, dtype=i32)[:, None] * 2 + near % 2
    is_near = cols < 16
    slots = jnp.arange(64, dtype=i32)[None]
    choice = z_rank * 8 + spot % NY
    code = jnp.where(is_near, near_place + 64 * 128, spot * 2 + choice * 128) + rows * 2**14 + slots * 2**15
    late = (~is_near) & (z_rank >= LATE_RANKS[0]) & (z_rank <= LATE_RANKS[-1])
    dead = slots >= counts[:, None]
    key = jnp.where(dead, 4, late.astype(i32) * 2 + rows) * 64 + slots
    position = jnp.sum((key[:, None, :] < key[:, :, None]).astype(i32), axis=2)
    code = jnp.sum(jnp.where(position[:, None, :] == slots[0][None, :, None], code[:, None, :], 0), axis=2)
    ends = jnp.arange(1, 5, dtype=i32)[:, None, None] * 64
    bounds = jnp.sum((key[None] < ends).astype(i32), axis=2)

    first_z = gather_z(first, 512)
    base = x_parts(gather_x(first[:1024], 2))

    def z_steps(step, *rings):
        return [part for (ahead, behind, _), rows, offset in rings for part in step_parts(ahead, behind, step, rows, offset)]

    ring = (first_z, 1024, 0)
    known = z_steps(1, ring) + z_steps(2, ring)
    sources = assemble([(first, 1024, 0), *known, *base], SOURCE_ROWS)
    lists = [assemble([(tile_values, 64, 0), (ahead_lists, 64, 64), (behind_lists, 64, 128)], 192)]
    lists.append(assemble([(far_low, 32, 0), (far_high, 32, 32)], 64))

    ahead, behind, far = first_z
    holders = [first, *ahead, far[1], *behind[::-1]]
    table = choices([None if rank in LATE_RANKS else holder for rank, holder in enumerate(holders)])
    sums = power([(0, 3)], "early", [code, bounds, table, groups, degrees], lists[:1], sources)
    notes = [code, bounds, choices(holders), groups, degrees]
    late = z_steps(3, ring) + far_parts(far, 512, 0)
    most = power([(0, 3)], "late", notes, lists[:1], None, late, sums)
    most_z = gather_z(most, 384)
    few = power([(3, 1)], "all", notes, lists[1:], sources, late)
    few_z = gather_z(few, 128)
    second = assemble([(most, 768, 0), (few, 256, 768)], 1024)
    base = x_parts(gather_x(second, 2))
    rings = (most_z, 768, 0), (few_z, 256, 768)
    known = z_steps(1, *rings) + z_steps(2, *rings)
    sources = assemble([(second, 1024, 0), *known, *base], SOURCE_ROWS)
    sums = power([(0, 3), (3, 1)], "early", notes, lists, sources, last=True)
    late = z_steps(3, *rings) + far_parts(most_z[2], 384, 0) + far_parts(few_z[2], 128, 768)
    logs_cut = power([(0, 3), (3, 1)], "late", notes, lists, None, late, sums, second, True)
    logs = jnp.zeros((256, 1024), bf16)
    for place, step in enumerate(POSITIONS):
        piece = logs_cut[place * 256 : place * 256 + 256]
        piece = ring_y(piece, -step) if step else piece
        logs = lax.dynamic_update_slice_in_dim(logs, piece, (y + step) % NY * 256, 1)
    contract = (((0,), (0,)), ((), ()))
    gram = jnp.zeros((128, 1024), jnp.float32)
    for rows in gather_x(logs, 3):
        columns = lax.dynamic_slice_in_dim(rows, rank * 128, 128, 1)
        gram += lax.dot_general(columns, rows, contract, preferred_element_type=jnp.float32)
    return logs, gram / 2048


def solution(mesh):
    placed = (
        P(("grp", "row"), None),
        P(("grp", "row")),
        P(("grp", "row"), None, None),
        P(("grp", "row")),
        P(("grp", "row")),
        P(("grp", "row")),
        P(("grp", "row"), None),
    )

    return jax.shard_map(
        step_body,
        mesh=mesh,
        in_specs=placed,
        out_specs=(P(("grp", "row"), None), P(("grp", "row"), None)),
        check_vma=False,
    )
```

```python
import functools

import jax
import jax.numpy as jnp
from jax import lax
from jax.experimental import pallas as pl
from jax.experimental.pallas import tpu as pltpu
from jax.sharding import PartitionSpec as P


NY, NZ, NX, NC = 4, 8, 4, 2


def y_pairs(step):
    return [(y * NZ + z, (y + step) % NY * NZ + z) for y in range(NY) for z in range(NZ)]


def z_pairs(step):
    return [(y * NZ + z, y * NZ + (z + step) % NZ) for y in range(NY) for z in range(NZ)]


def x_pairs(step):
    return [(x * NC + c, (x + step) % NX * NC + c) for x in range(NX) for c in range(NC)]


def core_pairs():
    return [(x * NC + c, x * NC + 1 - c) for x in range(NX) for c in range(NC)]


def ring_y(value, step):
    return lax.ppermute(value, "grp", y_pairs(step))


def ring_z(value, step):
    return lax.ppermute(value, "grp", z_pairs(step))


def ring_x(value, step):
    return lax.ppermute(value, "row", x_pairs(step))


def swap_core(value):
    return lax.ppermute(value, "row", core_pairs())


def gather_y(lists):
    ahead = ring_y(lists, 1)
    behind = ring_y(lists, -1)
    far_low = ring_y(assemble([(ahead, 32, 0)], 32), 1)
    far_high = ring_y(assemble([(behind, 32, 0)], 32, 32), -1)
    return ahead, behind, far_low, far_high


def gather_z(rows, half):
    ahead = behind = rows
    from_ahead, from_behind = [], []
    for _ in range(1, 4):
        ahead = ring_z(ahead, 1)
        behind = ring_z(behind, -1)
        from_ahead.append(ahead)
        from_behind.append(behind)
    far_first = ring_z(ahead[:half], 1)
    far_second = ring_z(behind[half:], -1)
    return from_ahead, from_behind, (far_first, far_second)


def gather_x(rows, swaps):
    height = rows.shape[0]
    half = height // 2
    ahead = ring_x(rows, 1)
    behind = ring_x(rows, -1)
    far_first = ring_x(ahead[:half], 1)
    far_second = ring_x(behind[half:], -1)
    own, near = [(rows, height, 0)], [(ahead, height, 0), (behind, height, height)]
    far = [(far_first, half, 0), (far_second, half, half)]
    if swaps == 3:
        mine = [rows, assemble(near, 2 * height), assemble(far, height)]
    else:
        near = own + [(piece, size, place + height) for piece, size, place in near]
        mine = [assemble(near, 3 * height), assemble(far, height)]
    theirs = []
    for block in mine:
        theirs.append(swap_core(block))
    return mine + theirs


POSITIONS = (0, 1, 3, 2)
SOURCE_ROWS = 16 * 1024
LATE_RANKS = (3, 4, 5)
SMEM = pl.BlockSpec(memory_space=pltpu.SMEM)
VMEM = pl.BlockSpec(memory_space=pltpu.VMEM)
ANY = pl.BlockSpec(memory_space=pl.ANY)
SMALL = pltpu.CompilerParams(vmem_limit_bytes=12 * 2**20)


def start_copies(pairs, sems, origin=0):
    copies = []
    for source, target, rows, place in pairs:
        copy = pltpu.make_async_copy(
            source.at[pl.ds(origin, rows)], target.at[pl.ds(place, rows)], sems.at[len(copies)]
        )
        copy.start()
        copies.append(copy)
    return copies


def assemble_body(spans, origin, *refs):
    pieces, out_ref, sems = refs[: len(spans)], refs[-2], refs[-1]
    for copy in start_copies([(piece, out_ref, *span) for piece, span in zip(pieces, spans)], sems, origin):
        copy.wait()


def assemble(parts, height, origin=0):
    pieces = [piece for piece, _, _ in parts]
    return pl.pallas_call(
        functools.partial(assemble_body, [(rows, place) for _, rows, place in parts], origin),
        in_specs=[ANY] * len(parts),
        out_specs=VMEM,
        out_shape=jax.ShapeDtypeStruct((height, *pieces[0].shape[1:]), pieces[0].dtype),
        scratch_shapes=[pltpu.SemaphoreType.DMA((len(parts),))],
        compiler_params=SMALL,
        cost_estimate=pl.CostEstimate(flops=300_000_000, bytes_accessed=2**22, transcendentals=0),
        name="assemble",
    )(*pieces)


def stack_body(*refs):
    pieces, out_ref, sems = refs[:4], refs[4], refs[5]
    copies = start_copies([(piece, out_ref, 256, 256 * k) for k, piece in enumerate(pieces)], sems)
    row_ids = lax.broadcasted_iota(jnp.int32, (16, 256), 0)
    notes = jnp.zeros((16, 256), jnp.float32)
    for k, piece in enumerate(pieces):
        line = piece[pl.ds(256, 16), :].astype(jnp.float32)[:1]
        notes = jnp.where(row_ids == k, jnp.broadcast_to(line, (16, 256)), notes)
    out_ref[pl.ds(1024, 16), :] = notes.astype(jnp.bfloat16)
    for copy in copies:
        copy.wait()


def stack(pieces):
    return pl.pallas_call(
        stack_body,
        in_specs=[VMEM] * 4,
        out_specs=VMEM,
        out_shape=jax.ShapeDtypeStruct((1040, 256), jnp.bfloat16),
        scratch_shapes=[pltpu.SemaphoreType.DMA((4,))],
        compiler_params=SMALL,
        cost_estimate=pl.CostEstimate(flops=100_000_000, bytes_accessed=2**20, transcendentals=0),
        name="stack",
    )(*pieces)


def choices_body(ranks, *refs):
    out_ref = refs[-1]
    out_ref[...] = jnp.zeros_like(out_ref)
    for ref, rank in zip(refs, ranks):
        lines = ref[ref.shape[0] - 16 :, 128:256].astype(jnp.float32)[:8]
        out_ref[rank * 8 : rank * 8 + 8, :] = lines.astype(jnp.int32)


def choices(holders):
    ranks = [rank for rank, holder in enumerate(holders) if holder is not None]
    return pl.pallas_call(
        functools.partial(choices_body, ranks),
        in_specs=[VMEM] * len(ranks),
        out_specs=VMEM,
        out_shape=jax.ShapeDtypeStruct((72, 128), jnp.int32),
        compiler_params=SMALL,
        cost_estimate=pl.CostEstimate(flops=100_000_000, bytes_accessed=2**16, transcendentals=0),
        name="choices",
    )(*[holders[rank] for rank in ranks])


LATE_FIRST = LATE_RANKS[0] * 1024


def power_body(plan, code_ref, bound_ref, table_ref, group_ref, degree_ref, *refs):
    groups, phase, last, spans = plan
    piece_refs, refs = refs[: len(spans)], refs[len(spans):]
    list_refs, refs = refs[: len(groups)], refs[len(groups):]
    x_ref = before_ref = sum_ref = None
    if phase != "late":
        x_ref, refs = refs[0], refs[1:]
    if phase == "late":
        sum_ref, refs = refs[0], refs[1:]
    if last and phase != "early":
        before_ref, refs = refs[0], refs[1:]
    out_ref, acc_ref, late_ref, sems = refs
    copies = start_copies([(piece, late_ref, *span) for piece, span in zip(piece_refs, spans)], sems)
    for copy in copies:
        copy.wait()

    def add_slots(member, list_ref, local, source_ref, origin, row, start, stop, chunk):
        group = group_ref[member]
        half = pl.ds(row * 128, 128)

        @pl.loop(0, (stop - start + chunk - 1) // chunk)
        def _(step):
            lefts, rights = [], []
            for k in range(chunk):
                place = start + step * chunk + k
                code = code_ref[member, jnp.minimum(place, 63)]
                live = place < stop
                source = ((code & 127) + table_ref[(code >> 7) & 127, group]) * 128 - origin
                source = pl.multiple_of(jnp.where(live, source, 0), 128)
                tile = list_ref[local * 64 + (code >> 15)]
                lefts.append(jnp.where(live, tile, jnp.zeros_like(tile)))
                rights.append(source_ref[pl.ds(source, 128), :])
            left = jnp.concatenate(lefts, axis=1)
            right = jnp.concatenate(rights, axis=0)
            acc_ref[half, :] += jnp.dot(left, right, preferred_element_type=jnp.float32)

    done = 0
    for (first, count), list_ref in zip(groups, list_refs):

        @pl.loop(0, count)
        def _(local, first=first, list_ref=list_ref, done=done):
            member = first + local
            base = (done + local) * 256
            here = pl.ds(pl.multiple_of(base, 256), 256)
            acc_ref[...] = sum_ref[here, :] if phase == "late" else jnp.zeros_like(acc_ref)
            ends = [0] + [bound_ref[k, member] for k in range(4)]
            for row in range(2):
                if phase != "late":
                    add_slots(member, list_ref, local, x_ref, 0, row, ends[row], ends[row + 1], 16)
                if phase != "early":
                    add_slots(member, list_ref, local, late_ref, LATE_FIRST, row, ends[row + 2], ends[row + 3], 8)
            if phase == "early":
                out_ref[here, :] = acc_ref[...]
                return
            for half in range(2):
                place = pl.ds(pl.multiple_of(base + half * 128, 128), 128)
                scale = jnp.broadcast_to(degree_ref[member][:1, half * 128 : half * 128 + 128], (128, 128)).T
                scale = jnp.concatenate([scale, scale], axis=1)
                value = (acc_ref[pl.ds(half * 128, 128), :] / scale).astype(jnp.bfloat16)
                if last:
                    total = before_ref[place, :].astype(jnp.float32) + value.astype(jnp.float32)
                    value = jnp.log(jnp.maximum(3.0 * total, 1.0)).astype(jnp.bfloat16)
                out_ref[place, :] = value

        done += count


def power(groups, phase, notes, lists, sources=None, late=(), sums=None, before=None, last=False):
    pieces = [piece for piece, _, _ in late]
    spans = [(rows, place - LATE_FIRST) for _, rows, place in late]
    extra = [value for value in (sources, sums, before) if value is not None]
    count = sum(count for _, count in groups)
    return pl.pallas_call(
        functools.partial(power_body, (groups, phase, last, spans)),
        in_specs=[SMEM] * 4 + [VMEM] + [ANY] * len(pieces) + [VMEM] * (len(lists) + len(extra)),
        out_specs=VMEM,
        out_shape=jax.ShapeDtypeStruct((count * 256, 256), jnp.float32 if phase == "early" else jnp.bfloat16),
        scratch_shapes=[
            pltpu.VMEM((256, 256), jnp.float32),
            pltpu.VMEM((len(LATE_RANKS) * 1024 if pieces else 16, 256), jnp.bfloat16),
            pltpu.SemaphoreType.DMA((max(len(pieces), 1),)),
        ],
        compiler_params=SMALL,
        cost_estimate=pl.CostEstimate(
            flops=count * 600_000_000, bytes_accessed=10 * 2**20, transcendentals=0
        ),
    )(*notes, *pieces, *lists, *extra)


def step_parts(ahead, behind, step, rows, offset):
    return [(ahead[step - 1], rows, step * 1024 + offset), (behind[step - 1], rows, (8 - step) * 1024 + offset)]


def x_parts(blocks):
    parts, place = [], 8192
    for block in blocks:
        parts.append((block, block.shape[0], place))
        place += block.shape[0]
    return parts


def far_parts(far, rows, offset):
    return [(far[0], rows, 4096 + offset), (far[1], rows, 4096 + offset + rows)]


def step_body(block, degree, tile_values, tile_rows, tile_cols, tile_count, send_tiles):
    bf16 = jnp.bfloat16
    i32 = jnp.int32
    group = lax.axis_index("grp")
    y, z = group // NZ, group % NZ
    rank = lax.axis_index("row")
    x, core = rank // NC, rank % NC
    extra = jnp.concatenate([tile_rows, tile_cols, send_tiles[0], tile_count, jnp.zeros((95,), i32), degree])
    extra = lax.optimization_barrier(extra.reshape(2, 256))
    extra = jnp.pad(extra, ((0, 14), (0, 0))).astype(bf16)
    pieces = []
    for step in POSITIONS:
        cut = lax.dynamic_slice_in_dim(block, (y + step) % NY * 256, 256, 1)
        cut = jnp.concatenate([cut, extra], axis=0)
        pieces.append(ring_y(cut, step) if step else cut)
    ahead_lists, behind_lists, far_low, far_high = gather_y(tile_values)
    first = stack(pieces)
    degrees = jnp.concatenate([piece[257:258] for piece in pieces], axis=0).astype(jnp.float32)
    degrees = jnp.broadcast_to(degrees[:, None, :], (NY, 8, 256))

    told = first[1024:1040].astype(i32)[:NY]
    rows, cols, counts = told[:, :64], told[:, 64:128], told[:, 160]
    steps = jnp.array(POSITIONS, i32)
    groups = (y - steps) % NY * NZ + z
    distant = jnp.maximum(cols - 16, 0)
    apart = (y - distant // NZ) % NY
    z_rank = (z - distant % NZ) % NZ
    spot = z_rank * NY + jnp.where(apart == 2, 3, jnp.where(apart == 3, 2, apart))
    near = jnp.minimum(cols, 15)
    near_rank = near // 2
    away = (x - near_rank // NC) % NX
    flip = (core + near_rank) % NC
    away = jnp.where(away == 2, 3, jnp.where(away == 3, 2, away))
    near_place = 64 + (flip * 4 + away) * 8 + jnp.arange(NY, dtype=i32)[:, None] * 2 + near % 2
    is_near = cols < 16
    slots = jnp.arange(64, dtype=i32)[None]
    choice = z_rank * 8 + spot % NY
    code = jnp.where(is_near, near_place + 64 * 128, spot * 2 + choice * 128) + rows * 2**14 + slots * 2**15
    late = (~is_near) & (z_rank >= LATE_RANKS[0]) & (z_rank <= LATE_RANKS[-1])
    dead = slots >= counts[:, None]
    key = jnp.where(dead, 4, late.astype(i32) * 2 + rows) * 64 + slots
    position = jnp.sum((key[:, None, :] < key[:, :, None]).astype(i32), axis=2)
    code = jnp.sum(jnp.where(position[:, None, :] == slots[0][None, :, None], code[:, None, :], 0), axis=2)
    ends = jnp.arange(1, 5, dtype=i32)[:, None, None] * 64
    bounds = jnp.sum((key[None] < ends).astype(i32), axis=2)

    first_z = gather_z(first, 512)
    base = x_parts(gather_x(first[:1024], 2))

    def z_steps(step, *rings):
        return [part for (ahead, behind, _), rows, offset in rings for part in step_parts(ahead, behind, step, rows, offset)]

    ring = (first_z, 1024, 0)
    known = z_steps(1, ring) + z_steps(2, ring)
    sources = assemble([(first, 1024, 0), *known, *base], SOURCE_ROWS)
    lists = [assemble([(tile_values, 64, 0), (ahead_lists, 64, 64), (behind_lists, 64, 128)], 192)]
    lists.append(assemble([(far_low, 32, 0), (far_high, 32, 32)], 64))

    ahead, behind, far = first_z
    holders = [first, *ahead, far[1], *behind[::-1]]
    table = choices([None if rank in LATE_RANKS else holder for rank, holder in enumerate(holders)])
    late_table = choices([holder if rank in LATE_RANKS else None for rank, holder in enumerate(holders)])
    sums = power([(0, 3)], "early", [code, bounds, table, groups, degrees], lists[:1], sources)
    late = z_steps(3, ring) + far_parts(far, 512, 0)
    most = power([(0, 3)], "late", [code, bounds, late_table, groups, degrees], lists[:1], None, late, sums)
    notes = [code, bounds, table + late_table, groups, degrees]
    most_z = gather_z(most, 384)
    few = power([(3, 1)], "all", notes, lists[1:], sources, late)
    few_z = gather_z(few, 128)
    second = assemble([(most, 768, 0), (few, 256, 768)], 1024)
    base = x_parts(gather_x(second, 2))
    rings = (most_z, 768, 0), (few_z, 256, 768)
    known = z_steps(1, *rings) + z_steps(2, *rings)
    sources = assemble([(second, 1024, 0), *known, *base], SOURCE_ROWS)
    sums = power([(0, 3), (3, 1)], "early", notes, lists, sources, last=True)
    late = z_steps(3, *rings) + far_parts(most_z[2], 384, 0) + far_parts(few_z[2], 128, 768)
    logs_cut = power([(0, 3), (3, 1)], "late", notes, lists, None, late, sums, second, True)
    logs = jnp.zeros((256, 1024), bf16)
    for place, step in enumerate(POSITIONS):
        piece = logs_cut[place * 256 : place * 256 + 256]
        piece = ring_y(piece, -step) if step else piece
        logs = lax.dynamic_update_slice_in_dim(logs, piece, (y + step) % NY * 256, 1)
    contract = (((0,), (0,)), ((), ()))
    blocks = gather_x(logs, 3)
    for number in range(6):
        rows = blocks[number // 2 + number % 2 * 3]
        columns = lax.dynamic_slice_in_dim(rows, rank * 128, 128, 1) * bf16(1 / 2048)
        product = lax.dot_general(columns, rows, contract, preferred_element_type=jnp.float32)
        gram = lax.optimization_barrier(gram) + product if number else product
    return logs, gram


def solution(mesh):
    placed = (
        P(("grp", "row"), None),
        P(("grp", "row")),
        P(("grp", "row"), None, None),
        P(("grp", "row")),
        P(("grp", "row")),
        P(("grp", "row")),
        P(("grp", "row"), None),
    )

    return jax.shard_map(
        step_body,
        mesh=mesh,
        in_specs=placed,
        out_specs=(P(("grp", "row"), None), P(("grp", "row"), None)),
        check_vma=False,
    )
```

```python
import functools

import jax
import jax.numpy as jnp
from jax import lax
from jax.experimental import pallas as pl
from jax.experimental.pallas import tpu as pltpu
from jax.sharding import PartitionSpec as P


NY, NZ, NX, NC = 4, 8, 4, 2


def y_pairs(step):
    return [(y * NZ + z, (y + step) % NY * NZ + z) for y in range(NY) for z in range(NZ)]


def z_pairs(step):
    return [(y * NZ + z, y * NZ + (z + step) % NZ) for y in range(NY) for z in range(NZ)]


def x_pairs(step):
    return [(x * NC + c, (x + step) % NX * NC + c) for x in range(NX) for c in range(NC)]


def core_pairs():
    return [(x * NC + c, x * NC + 1 - c) for x in range(NX) for c in range(NC)]


def ring_y(value, step):
    return lax.ppermute(value, "grp", y_pairs(step))


def ring_z(value, step):
    return lax.ppermute(value, "grp", z_pairs(step))


def ring_x(value, step):
    return lax.ppermute(value, "row", x_pairs(step))


def swap_core(value):
    return lax.ppermute(value, "row", core_pairs())


def gather_y(lists):
    ahead = ring_y(lists, 1)
    behind = ring_y(lists, -1)
    far_low = ring_y(assemble([(ahead, 32, 0)], 32), 1)
    far_high = ring_y(assemble([(behind, 32, 0)], 32, 32), -1)
    return ahead, behind, far_low, far_high


def gather_z(rows, half):
    ahead = behind = rows
    from_ahead, from_behind = [], []
    for _ in range(1, 4):
        ahead = ring_z(ahead, 1)
        behind = ring_z(behind, -1)
        from_ahead.append(ahead)
        from_behind.append(behind)
    far_first = ring_z(ahead[:half], 1)
    far_second = ring_z(behind[half:], -1)
    return from_ahead, from_behind, (far_first, far_second)


def gather_x(rows, swaps):
    height = rows.shape[0]
    half = height // 2
    ahead = ring_x(rows, 1)
    behind = ring_x(rows, -1)
    far_first = assemble([(ahead, half, 0)], half)
    far_second = assemble([(behind, half, 0)], half, half)
    far_first = ring_x(far_first, 1)
    far_second = ring_x(far_second, -1)
    own, near = [(rows, height, 0)], [(ahead, height, 0), (behind, height, height)]
    far = [(far_first, half, 0), (far_second, half, half)]
    if swaps == 3:
        mine = [rows, assemble(near, 2 * height), assemble(far, height)]
    else:
        near = own + [(piece, size, place + height) for piece, size, place in near]
        mine = [assemble(near, 3 * height)]
        mine.append(assemble(far, height))
    theirs = []
    for block in mine:
        theirs.append(swap_core(block))
    return mine + theirs


POSITIONS = (0, 1, 3, 2)
SOURCE_ROWS = 16 * 1024
LATE_RANKS = (3, 4, 5)
SMEM = pl.BlockSpec(memory_space=pltpu.SMEM)
VMEM = pl.BlockSpec(memory_space=pltpu.VMEM)
ANY = pl.BlockSpec(memory_space=pl.ANY)
SMALL = pltpu.CompilerParams(vmem_limit_bytes=12 * 2**20)


def start_copies(pairs, sems, origin=0):
    copies = []
    for source, target, rows, place in pairs:
        copy = pltpu.make_async_copy(
            source.at[pl.ds(origin, rows)], target.at[pl.ds(place, rows)], sems.at[len(copies)]
        )
        copy.start()
        copies.append(copy)
    return copies


def assemble_body(spans, origin, *refs):
    pieces, out_ref, sems = refs[: len(spans)], refs[-2], refs[-1]
    for copy in start_copies([(piece, out_ref, *span) for piece, span in zip(pieces, spans)], sems, origin):
        copy.wait()


def assemble(parts, height, origin=0):
    pieces = [piece for piece, _, _ in parts]
    return pl.pallas_call(
        functools.partial(assemble_body, [(rows, place) for _, rows, place in parts], origin),
        in_specs=[ANY] * len(parts),
        out_specs=VMEM,
        out_shape=jax.ShapeDtypeStruct((height, *pieces[0].shape[1:]), pieces[0].dtype),
        scratch_shapes=[pltpu.SemaphoreType.DMA((len(parts),))],
        compiler_params=SMALL,
        cost_estimate=pl.CostEstimate(flops=300_000_000, bytes_accessed=2**22, transcendentals=0),
        name="assemble",
    )(*pieces)


def stack_body(*refs):
    pieces, out_ref, sems = refs[:4], refs[4], refs[5]
    copies = start_copies([(piece, out_ref, 256, 256 * k) for k, piece in enumerate(pieces)], sems)
    row_ids = lax.broadcasted_iota(jnp.int32, (16, 256), 0)
    notes = jnp.zeros((16, 256), jnp.float32)
    for k, piece in enumerate(pieces):
        line = piece[pl.ds(256, 16), :].astype(jnp.float32)[:1]
        notes = jnp.where(row_ids == k, jnp.broadcast_to(line, (16, 256)), notes)
    out_ref[pl.ds(1024, 16), :] = notes.astype(jnp.bfloat16)
    for copy in copies:
        copy.wait()


def stack(pieces):
    return pl.pallas_call(
        stack_body,
        in_specs=[VMEM] * 4,
        out_specs=VMEM,
        out_shape=jax.ShapeDtypeStruct((1040, 256), jnp.bfloat16),
        scratch_shapes=[pltpu.SemaphoreType.DMA((4,))],
        compiler_params=SMALL,
        cost_estimate=pl.CostEstimate(flops=100_000_000, bytes_accessed=2**20, transcendentals=0),
        name="stack",
    )(*pieces)


def choices_body(ranks, *refs):
    out_ref = refs[-1]
    out_ref[...] = jnp.zeros_like(out_ref)
    for ref, rank in zip(refs, ranks):
        lines = ref[ref.shape[0] - 16 :, 128:256].astype(jnp.float32)[:8]
        out_ref[rank * 8 : rank * 8 + 8, :] = lines.astype(jnp.int32)


def choices(holders):
    ranks = [rank for rank, holder in enumerate(holders) if holder is not None]
    return pl.pallas_call(
        functools.partial(choices_body, ranks),
        in_specs=[VMEM] * len(ranks),
        out_specs=VMEM,
        out_shape=jax.ShapeDtypeStruct((72, 128), jnp.int32),
        compiler_params=SMALL,
        cost_estimate=pl.CostEstimate(flops=100_000_000, bytes_accessed=2**16, transcendentals=0),
        name="choices",
    )(*[holders[rank] for rank in ranks])


LATE_FIRST = LATE_RANKS[0] * 1024


def power_body(plan, code_ref, bound_ref, table_ref, group_ref, degree_ref, *refs):
    groups, phase, last, spans = plan
    piece_refs, refs = refs[: len(spans)], refs[len(spans):]
    list_refs, refs = refs[: len(groups)], refs[len(groups):]
    x_ref = before_ref = sum_ref = None
    if phase != "late":
        x_ref, refs = refs[0], refs[1:]
    if phase == "late":
        sum_ref, refs = refs[0], refs[1:]
    if last and phase != "early":
        before_ref, refs = refs[0], refs[1:]
    out_ref, acc_ref, late_ref, sems = refs
    copies = start_copies([(piece, late_ref, *span) for piece, span in zip(piece_refs, spans)], sems)
    for copy in copies:
        copy.wait()

    def add_slots(member, list_ref, local, source_ref, origin, row, start, stop, chunk):
        group = group_ref[member]
        half = pl.ds(row * 128, 128)

        @pl.loop(0, (stop - start + chunk - 1) // chunk)
        def _(step):
            lefts, rights = [], []
            for k in range(chunk):
                place = start + step * chunk + k
                code = code_ref[member, jnp.minimum(place, 63)]
                live = place < stop
                source = ((code & 127) + table_ref[(code >> 7) & 127, group]) * 128 - origin
                source = pl.multiple_of(jnp.where(live, source, 0), 128)
                tile = list_ref[local * 64 + (code >> 15)]
                lefts.append(jnp.where(live, tile, jnp.zeros_like(tile)))
                rights.append(source_ref[pl.ds(source, 128), :])
            left = jnp.concatenate(lefts, axis=1)
            right = jnp.concatenate(rights, axis=0)
            acc_ref[half, :] += jnp.dot(left, right, preferred_element_type=jnp.float32)

    done = 0
    for (first, count), list_ref in zip(groups, list_refs):

        @pl.loop(0, count)
        def _(local, first=first, list_ref=list_ref, done=done):
            member = first + local
            base = (done + local) * 256
            here = pl.ds(pl.multiple_of(base, 256), 256)
            acc_ref[...] = sum_ref[here, :] if phase == "late" else jnp.zeros_like(acc_ref)
            ends = [0] + [bound_ref[k, member] for k in range(4)]
            for row in range(2):
                if phase != "late":
                    add_slots(member, list_ref, local, x_ref, 0, row, ends[row], ends[row + 1], 16)
                if phase != "early":
                    add_slots(member, list_ref, local, late_ref, LATE_FIRST, row, ends[row + 2], ends[row + 3], 8)
            if phase == "early":
                out_ref[here, :] = acc_ref[...]
                return
            for half in range(2):
                place = pl.ds(pl.multiple_of(base + half * 128, 128), 128)
                scale = jnp.broadcast_to(degree_ref[member][:1, half * 128 : half * 128 + 128], (128, 128)).T
                scale = jnp.concatenate([scale, scale], axis=1)
                value = (acc_ref[pl.ds(half * 128, 128), :] / scale).astype(jnp.bfloat16)
                if last:
                    total = before_ref[place, :].astype(jnp.float32) + value.astype(jnp.float32)
                    value = jnp.log(jnp.maximum(3.0 * total, 1.0)).astype(jnp.bfloat16)
                out_ref[place, :] = value

        done += count


def power(groups, phase, notes, lists, sources=None, late=(), sums=None, before=None, last=False):
    pieces = [piece for piece, _, _ in late]
    spans = [(rows, place - LATE_FIRST) for _, rows, place in late]
    extra = [value for value in (sources, sums, before) if value is not None]
    count = sum(count for _, count in groups)
    return pl.pallas_call(
        functools.partial(power_body, (groups, phase, last, spans)),
        in_specs=[SMEM] * 4 + [VMEM] + [ANY] * len(pieces) + [VMEM] * (len(lists) + len(extra)),
        out_specs=VMEM,
        out_shape=jax.ShapeDtypeStruct((count * 256, 256), jnp.float32 if phase == "early" else jnp.bfloat16),
        scratch_shapes=[
            pltpu.VMEM((256, 256), jnp.float32),
            pltpu.VMEM((len(LATE_RANKS) * 1024 if pieces else 16, 256), jnp.bfloat16),
            pltpu.SemaphoreType.DMA((max(len(pieces), 1),)),
        ],
        compiler_params=SMALL,
        cost_estimate=pl.CostEstimate(
            flops=count * 600_000_000, bytes_accessed=10 * 2**20, transcendentals=0
        ),
    )(*notes, *pieces, *lists, *extra)


def step_parts(ahead, behind, step, rows, offset):
    return [(ahead[step - 1], rows, step * 1024 + offset), (behind[step - 1], rows, (8 - step) * 1024 + offset)]


def x_parts(blocks):
    parts, place = [], 8192
    for block in blocks:
        parts.append((block, block.shape[0], place))
        place += block.shape[0]
    return parts


def far_parts(far, rows, offset):
    return [(far[0], rows, 4096 + offset), (far[1], rows, 4096 + offset + rows)]


def step_body(block, degree, tile_values, tile_rows, tile_cols, tile_count, send_tiles):
    bf16 = jnp.bfloat16
    i32 = jnp.int32
    group = lax.axis_index("grp")
    y, z = group // NZ, group % NZ
    rank = lax.axis_index("row")
    x, core = rank // NC, rank % NC
    extra = jnp.concatenate([tile_rows, tile_cols, send_tiles[0], tile_count, jnp.zeros((95,), i32), degree])
    extra = lax.optimization_barrier(extra.reshape(2, 256))
    extra = jnp.pad(extra, ((0, 14), (0, 0))).astype(bf16)
    pieces = []
    for step in POSITIONS:
        cut = lax.dynamic_slice_in_dim(block, (y + step) % NY * 256, 256, 1)
        cut = jnp.concatenate([cut, extra], axis=0)
        pieces.append(ring_y(cut, step) if step else cut)
    ahead_lists, behind_lists, far_low, far_high = gather_y(tile_values)
    first = stack(pieces)
    degrees = jnp.concatenate([piece[257:258] for piece in pieces], axis=0).astype(jnp.float32)
    degrees = jnp.broadcast_to(degrees[:, None, :], (NY, 8, 256))

    told = first[1024:1040].astype(i32)[:NY]
    rows, cols, counts = told[:, :64], told[:, 64:128], told[:, 160]
    steps = jnp.array(POSITIONS, i32)
    groups = (y - steps) % NY * NZ + z
    distant = jnp.maximum(cols - 16, 0)
    apart = (y - distant // NZ) % NY
    z_rank = (z - distant % NZ) % NZ
    spot = z_rank * NY + jnp.where(apart == 2, 3, jnp.where(apart == 3, 2, apart))
    near = jnp.minimum(cols, 15)
    near_rank = near // 2
    away = (x - near_rank // NC) % NX
    flip = (core + near_rank) % NC
    away = jnp.where(away == 2, 3, jnp.where(away == 3, 2, away))
    near_place = 64 + (flip * 4 + away) * 8 + jnp.arange(NY, dtype=i32)[:, None] * 2 + near % 2
    is_near = cols < 16
    slots = jnp.arange(64, dtype=i32)[None]
    choice = z_rank * 8 + spot % NY
    code = jnp.where(is_near, near_place + 64 * 128, spot * 2 + choice * 128) + rows * 2**14 + slots * 2**15
    late = (~is_near) & (z_rank >= LATE_RANKS[0]) & (z_rank <= LATE_RANKS[-1])
    dead = slots >= counts[:, None]
    key = jnp.where(dead, 4, late.astype(i32) * 2 + rows) * 64 + slots
    position = jnp.sum((key[:, None, :] < key[:, :, None]).astype(i32), axis=2)
    code = jnp.sum(jnp.where(position[:, None, :] == slots[0][None, :, None], code[:, None, :], 0), axis=2)
    ends = jnp.arange(1, 5, dtype=i32)[:, None, None] * 64
    bounds = jnp.sum((key[None] < ends).astype(i32), axis=2)

    first_z = gather_z(first, 512)
    base = x_parts(gather_x(first[:1024], 2))

    def z_steps(step, *rings):
        return [part for (ahead, behind, _), rows, offset in rings for part in step_parts(ahead, behind, step, rows, offset)]

    ring = (first_z, 1024, 0)
    known = z_steps(1, ring) + z_steps(2, ring)
    sources = assemble([(first, 1024, 0), *known, *base], SOURCE_ROWS)
    lists = [assemble([(tile_values, 64, 0), (ahead_lists, 64, 64), (behind_lists, 64, 128)], 192)]
    lists.append(assemble([(far_low, 32, 0), (far_high, 32, 32)], 64))

    ahead, behind, far = first_z
    holders = [first, *ahead, far[1], *behind[::-1]]
    table = choices([None if rank in LATE_RANKS else holder for rank, holder in enumerate(holders)])
    late_table = choices([holder if rank in LATE_RANKS else None for rank, holder in enumerate(holders)])
    sums = power([(0, 3)], "early", [code, bounds, table, groups, degrees], lists[:1], sources)
    late = z_steps(3, ring) + far_parts(far, 512, 0)
    most = power([(0, 3)], "late", [code, bounds, late_table, groups, degrees], lists[:1], None, late, sums)
    notes = [code, bounds, table + late_table, groups, degrees]
    most_z = gather_z(most, 384)
    few = power([(3, 1)], "all", notes, lists[1:], sources, late)
    few_z = gather_z(few, 128)
    second = assemble([(most, 768, 0), (few, 256, 768)], 1024)
    base = x_parts(gather_x(second, 2))
    rings = (most_z, 768, 0), (few_z, 256, 768)
    known = z_steps(1, *rings) + z_steps(2, *rings)
    sources = assemble([(second, 1024, 0), *known, *base], SOURCE_ROWS)
    sums = power([(0, 3), (3, 1)], "early", notes, lists, sources, last=True)
    late = z_steps(3, *rings) + far_parts(most_z[2], 384, 0) + far_parts(few_z[2], 128, 768)
    logs_cut = power([(0, 3), (3, 1)], "late", notes, lists, None, late, sums, second, True)
    logs = jnp.zeros((256, 1024), bf16)
    for place, step in enumerate(POSITIONS):
        piece = logs_cut[place * 256 : place * 256 + 256]
        piece = ring_y(piece, -step) if step else piece
        logs = lax.dynamic_update_slice_in_dim(logs, piece, (y + step) % NY * 256, 1)
    contract = (((0,), (0,)), ((), ()))
    blocks = gather_x(logs, 3)
    for number, place in enumerate((5, 0, 3, 1, 4, 2)):
        rows = blocks[place]
        columns = lax.dynamic_slice_in_dim(rows, rank * 128, 128, 1) * bf16(1 / 2048)
        product = lax.dot_general(columns, rows, contract, preferred_element_type=jnp.float32)
        gram = gram + product if number else product
    return logs, gram


def solution(mesh):
    placed = (
        P(("grp", "row"), None),
        P(("grp", "row")),
        P(("grp", "row"), None, None),
        P(("grp", "row")),
        P(("grp", "row")),
        P(("grp", "row")),
        P(("grp", "row"), None),
    )

    return jax.shard_map(
        step_body,
        mesh=mesh,
        in_specs=placed,
        out_specs=(P(("grp", "row"), None), P(("grp", "row"), None)),
        check_vma=False,
    )
```

```python
import functools

import jax
import jax.numpy as jnp
from jax import lax
from jax.experimental import pallas as pl
from jax.experimental.pallas import tpu as pltpu
from jax.sharding import PartitionSpec as P


NY, NZ, NX, NC = 4, 8, 4, 2


def y_pairs(step):
    return [(y * NZ + z, (y + step) % NY * NZ + z) for y in range(NY) for z in range(NZ)]


def z_pairs(step):
    return [(y * NZ + z, y * NZ + (z + step) % NZ) for y in range(NY) for z in range(NZ)]


def x_pairs(step):
    return [(x * NC + c, (x + step) % NX * NC + c) for x in range(NX) for c in range(NC)]


def core_pairs():
    return [(x * NC + c, x * NC + 1 - c) for x in range(NX) for c in range(NC)]


def ring_y(value, step):
    return lax.ppermute(value, "grp", y_pairs(step))


def ring_z(value, step):
    return lax.ppermute(value, "grp", z_pairs(step))


def ring_x(value, step):
    return lax.ppermute(value, "row", x_pairs(step))


def swap_core(value):
    return lax.ppermute(value, "row", core_pairs())


def gather_y(lists):
    ahead = ring_y(lists, 1)
    behind = ring_y(lists, -1)
    far_low = ring_y(assemble([(ahead, 32, 0)], 32), 1)
    far_high = ring_y(assemble([(behind, 32, 0)], 32, 32), -1)
    return ahead, behind, far_low, far_high


def gather_z(rows, half):
    ahead = behind = rows
    from_ahead, from_behind = [], []
    for _ in range(1, 4):
        ahead = ring_z(ahead, 1)
        behind = ring_z(behind, -1)
        from_ahead.append(ahead)
        from_behind.append(behind)
    far_first = ring_z(ahead[:half], 1)
    far_second = ring_z(behind[half:], -1)
    return from_ahead, from_behind, (far_first, far_second)


def gather_x(rows, swaps):
    height = rows.shape[0]
    half = height // 2
    ahead = ring_x(rows, 1)
    behind = ring_x(rows, -1)
    far_first = ring_x(ahead[:half], 1)
    far_second = ring_x(behind[half:], -1)
    own, near = [(rows, height, 0)], [(ahead, height, 0), (behind, height, height)]
    far = [(far_first, half, 0), (far_second, half, half)]
    if swaps == 3:
        mine = [rows, assemble(near, 2 * height), assemble(far, height)]
    else:
        near = own + [(piece, size, place + height) for piece, size, place in near]
        mine = [assemble(near, 3 * height), assemble(far, height)]
    theirs = []
    for block in mine:
        theirs.append(swap_core(block))
    return mine + theirs


POSITIONS = (0, 1, 3, 2)
SOURCE_ROWS = 16 * 1024
LATE_RANKS = (3, 4, 5)
SMEM = pl.BlockSpec(memory_space=pltpu.SMEM)
VMEM = pl.BlockSpec(memory_space=pltpu.VMEM)
ANY = pl.BlockSpec(memory_space=pl.ANY)
SMALL = pltpu.CompilerParams(vmem_limit_bytes=12 * 2**20)


def start_copies(pairs, sems, origin=0):
    copies = []
    for source, target, rows, place in pairs:
        copy = pltpu.make_async_copy(
            source.at[pl.ds(origin, rows)], target.at[pl.ds(place, rows)], sems.at[len(copies)]
        )
        copy.start()
        copies.append(copy)
    return copies


def assemble_body(spans, origin, *refs):
    pieces, out_ref, sems = refs[: len(spans)], refs[-2], refs[-1]
    for copy in start_copies([(piece, out_ref, *span) for piece, span in zip(pieces, spans)], sems, origin):
        copy.wait()


def assemble(parts, height, origin=0):
    pieces = [piece for piece, _, _ in parts]
    return pl.pallas_call(
        functools.partial(assemble_body, [(rows, place) for _, rows, place in parts], origin),
        in_specs=[ANY] * len(parts),
        out_specs=VMEM,
        out_shape=jax.ShapeDtypeStruct((height, *pieces[0].shape[1:]), pieces[0].dtype),
        scratch_shapes=[pltpu.SemaphoreType.DMA((len(parts),))],
        compiler_params=SMALL,
        cost_estimate=pl.CostEstimate(flops=300_000_000, bytes_accessed=2**22, transcendentals=0),
        name="assemble",
    )(*pieces)


def stack_body(*refs):
    pieces, out_ref, sems = refs[:4], refs[4], refs[5]
    copies = start_copies([(piece, out_ref, 256, 256 * k) for k, piece in enumerate(pieces)], sems)
    row_ids = lax.broadcasted_iota(jnp.int32, (16, 256), 0)
    notes = jnp.zeros((16, 256), jnp.float32)
    for k, piece in enumerate(pieces):
        line = piece[pl.ds(256, 16), :].astype(jnp.float32)[:1]
        notes = jnp.where(row_ids == k, jnp.broadcast_to(line, (16, 256)), notes)
    out_ref[pl.ds(1024, 16), :] = notes.astype(jnp.bfloat16)
    for copy in copies:
        copy.wait()


def stack(pieces):
    return pl.pallas_call(
        stack_body,
        in_specs=[VMEM] * 4,
        out_specs=VMEM,
        out_shape=jax.ShapeDtypeStruct((1040, 256), jnp.bfloat16),
        scratch_shapes=[pltpu.SemaphoreType.DMA((4,))],
        compiler_params=SMALL,
        cost_estimate=pl.CostEstimate(flops=100_000_000, bytes_accessed=2**20, transcendentals=0),
        name="stack",
    )(*pieces)


def choices_body(ranks, *refs):
    out_ref = refs[-1]
    out_ref[...] = jnp.zeros_like(out_ref)
    for ref, rank in zip(refs, ranks):
        lines = ref[ref.shape[0] - 16 :, 128:256].astype(jnp.float32)[:8]
        out_ref[rank * 8 : rank * 8 + 8, :] = lines.astype(jnp.int32)


def choices(holders):
    ranks = [rank for rank, holder in enumerate(holders) if holder is not None]
    return pl.pallas_call(
        functools.partial(choices_body, ranks),
        in_specs=[VMEM] * len(ranks),
        out_specs=VMEM,
        out_shape=jax.ShapeDtypeStruct((72, 128), jnp.int32),
        compiler_params=SMALL,
        cost_estimate=pl.CostEstimate(flops=100_000_000, bytes_accessed=2**16, transcendentals=0),
        name="choices",
    )(*[holders[rank] for rank in ranks])


LATE_FIRST = LATE_RANKS[0] * 1024


def power_body(plan, code_ref, bound_ref, table_ref, group_ref, degree_ref, *refs):
    groups, phase, last, spans = plan
    piece_refs, refs = refs[: len(spans)], refs[len(spans):]
    list_refs, refs = refs[: len(groups)], refs[len(groups):]
    x_ref = before_ref = sum_ref = None
    if phase != "late":
        x_ref, refs = refs[0], refs[1:]
    if phase == "late":
        sum_ref, refs = refs[0], refs[1:]
    if last and phase != "early":
        before_ref, refs = refs[0], refs[1:]
    out_ref, acc_ref, late_ref, sems = refs
    copies = start_copies([(piece, late_ref, *span) for piece, span in zip(piece_refs, spans)], sems)
    for copy in copies:
        copy.wait()

    def add_slots(member, list_ref, local, source_ref, origin, row, start, stop, chunk):
        group = group_ref[member]
        half = pl.ds(row * 128, 128)

        @pl.loop(0, (stop - start + chunk - 1) // chunk)
        def _(step):
            lefts, rights = [], []
            for k in range(chunk):
                place = start + step * chunk + k
                code = code_ref[member, jnp.minimum(place, 63)]
                live = place < stop
                source = ((code & 127) + table_ref[(code >> 7) & 127, group]) * 128 - origin
                source = pl.multiple_of(jnp.where(live, source, 0), 128)
                tile = list_ref[local * 64 + (code >> 15)]
                lefts.append(jnp.where(live, tile, jnp.zeros_like(tile)))
                rights.append(source_ref[pl.ds(source, 128), :])
            left = jnp.concatenate(lefts, axis=1)
            right = jnp.concatenate(rights, axis=0)
            acc_ref[half, :] += jnp.dot(left, right, preferred_element_type=jnp.float32)

    done = 0
    for (first, count), list_ref in zip(groups, list_refs):

        @pl.loop(0, count)
        def _(local, first=first, list_ref=list_ref, done=done):
            member = first + local
            base = (done + local) * 256
            here = pl.ds(pl.multiple_of(base, 256), 256)
            acc_ref[...] = sum_ref[here, :] if phase == "late" else jnp.zeros_like(acc_ref)
            ends = [0] + [bound_ref[k, member] for k in range(4)]
            for row in range(2):
                if phase != "late":
                    add_slots(member, list_ref, local, x_ref, 0, row, ends[row], ends[row + 1], 16)
                if phase != "early":
                    add_slots(member, list_ref, local, late_ref, LATE_FIRST, row, ends[row + 2], ends[row + 3], 8)
            if phase == "early":
                out_ref[here, :] = acc_ref[...]
                return
            for half in range(2):
                place = pl.ds(pl.multiple_of(base + half * 128, 128), 128)
                scale = jnp.broadcast_to(degree_ref[member][:1, half * 128 : half * 128 + 128], (128, 128)).T
                scale = jnp.concatenate([scale, scale], axis=1)
                value = (acc_ref[pl.ds(half * 128, 128), :] / scale).astype(jnp.bfloat16)
                if last:
                    total = before_ref[place, :].astype(jnp.float32) + value.astype(jnp.float32)
                    value = jnp.log(jnp.maximum(3.0 * total, 1.0)).astype(jnp.bfloat16)
                out_ref[place, :] = value

        done += count


def power(groups, phase, notes, lists, sources=None, late=(), sums=None, before=None, last=False):
    pieces = [piece for piece, _, _ in late]
    spans = [(rows, place - LATE_FIRST) for _, rows, place in late]
    extra = [value for value in (sources, sums, before) if value is not None]
    count = sum(count for _, count in groups)
    return pl.pallas_call(
        functools.partial(power_body, (groups, phase, last, spans)),
        in_specs=[SMEM] * 4 + [VMEM] + [ANY] * len(pieces) + [VMEM] * (len(lists) + len(extra)),
        out_specs=VMEM,
        out_shape=jax.ShapeDtypeStruct((count * 256, 256), jnp.float32 if phase == "early" else jnp.bfloat16),
        scratch_shapes=[
            pltpu.VMEM((256, 256), jnp.float32),
            pltpu.VMEM((len(LATE_RANKS) * 1024 if pieces else 16, 256), jnp.bfloat16),
            pltpu.SemaphoreType.DMA((max(len(pieces), 1),)),
        ],
        compiler_params=SMALL,
        cost_estimate=pl.CostEstimate(
            flops=count * 600_000_000, bytes_accessed=10 * 2**20, transcendentals=0
        ),
    )(*notes, *pieces, *lists, *extra)


def step_parts(ahead, behind, step, rows, offset):
    return [(ahead[step - 1], rows, step * 1024 + offset), (behind[step - 1], rows, (8 - step) * 1024 + offset)]


def x_parts(blocks):
    parts, place = [], 8192
    for block in blocks:
        parts.append((block, block.shape[0], place))
        place += block.shape[0]
    return parts


def far_parts(far, rows, offset):
    return [(far[0], rows, 4096 + offset), (far[1], rows, 4096 + offset + rows)]


def step_body(block, degree, tile_values, tile_rows, tile_cols, tile_count, send_tiles):
    bf16 = jnp.bfloat16
    i32 = jnp.int32
    group = lax.axis_index("grp")
    y, z = group // NZ, group % NZ
    rank = lax.axis_index("row")
    x, core = rank // NC, rank % NC
    extra = jnp.concatenate([tile_rows, tile_cols, send_tiles[0], tile_count, jnp.zeros((95,), i32), degree])
    extra = lax.optimization_barrier(extra.reshape(2, 256))
    extra = jnp.pad(extra, ((0, 14), (0, 0))).astype(bf16)
    pieces = []
    for step in POSITIONS:
        cut = lax.dynamic_slice_in_dim(block, (y + step) % NY * 256, 256, 1)
        cut = jnp.concatenate([cut, extra], axis=0)
        pieces.append(ring_y(cut, step) if step else cut)
    ahead_lists, behind_lists, far_low, far_high = gather_y(tile_values)
    first = stack(pieces)
    degrees = jnp.concatenate([piece[257:258] for piece in pieces], axis=0).astype(jnp.float32)
    degrees = jnp.broadcast_to(degrees[:, None, :], (NY, 8, 256))

    told = first[1024:1040].astype(i32)[:NY]
    rows, cols, counts = told[:, :64], told[:, 64:128], told[:, 160]
    steps = jnp.array(POSITIONS, i32)
    groups = (y - steps) % NY * NZ + z
    distant = jnp.maximum(cols - 16, 0)
    apart = (y - distant // NZ) % NY
    z_rank = (z - distant % NZ) % NZ
    spot = z_rank * NY + jnp.where(apart == 2, 3, jnp.where(apart == 3, 2, apart))
    near = jnp.minimum(cols, 15)
    near_rank = near // 2
    away = (x - near_rank // NC) % NX
    flip = (core + near_rank) % NC
    away = jnp.where(away == 2, 3, jnp.where(away == 3, 2, away))
    near_place = 64 + (flip * 4 + away) * 8 + jnp.arange(NY, dtype=i32)[:, None] * 2 + near % 2
    is_near = cols < 16
    slots = jnp.arange(64, dtype=i32)[None]
    choice = z_rank * 8 + spot % NY
    code = jnp.where(is_near, near_place + 64 * 128, spot * 2 + choice * 128) + rows * 2**14 + slots * 2**15
    late = (~is_near) & (z_rank >= LATE_RANKS[0]) & (z_rank <= LATE_RANKS[-1])
    dead = slots >= counts[:, None]
    key = jnp.where(dead, 4, late.astype(i32) * 2 + rows) * 64 + slots
    position = jnp.sum((key[:, None, :] < key[:, :, None]).astype(i32), axis=2)
    code = jnp.sum(jnp.where(position[:, None, :] == slots[0][None, :, None], code[:, None, :], 0), axis=2)
    ends = jnp.arange(1, 5, dtype=i32)[:, None, None] * 64
    bounds = jnp.sum((key[None] < ends).astype(i32), axis=2)

    first_z = gather_z(first, 512)
    base = x_parts(gather_x(first[:1024], 2))

    def z_steps(step, *rings):
        return [part for (ahead, behind, _), rows, offset in rings for part in step_parts(ahead, behind, step, rows, offset)]

    ring = (first_z, 1024, 0)
    known = z_steps(1, ring) + z_steps(2, ring)
    sources = assemble([(first, 1024, 0), *known, *base], SOURCE_ROWS)
    lists = [assemble([(tile_values, 64, 0), (ahead_lists, 64, 64), (behind_lists, 64, 128)], 192)]
    lists.append(assemble([(far_low, 32, 0), (far_high, 32, 32)], 64))

    ahead, behind, far = first_z
    holders = [first, *ahead, far[1], *behind[::-1]]
    table = choices([None if rank in LATE_RANKS else holder for rank, holder in enumerate(holders)])
    sums = power([(0, 3)], "early", [code, bounds, table, groups, degrees], lists[:1], sources)
    late_table = choices([holder if rank in LATE_RANKS else None for rank, holder in enumerate(holders)])
    late = z_steps(3, ring) + far_parts(far, 512, 0)
    most = power([(0, 3)], "late", [code, bounds, late_table, groups, degrees], lists[:1], None, late, sums)
    notes = [code, bounds, table + late_table, groups, degrees]
    most_z = gather_z(most, 384)
    few = power([(3, 1)], "all", notes, lists[1:], sources, late)
    few_z = gather_z(few, 128)
    second = assemble([(most, 768, 0), (few, 256, 768)], 1024)
    base = x_parts(gather_x(second, 2))
    rings = (most_z, 768, 0), (few_z, 256, 768)
    known = z_steps(1, *rings) + z_steps(2, *rings)
    sources = assemble([(second, 1024, 0), *known, *base], SOURCE_ROWS)
    sums = power([(0, 3), (3, 1)], "early", notes, lists, sources, last=True)
    late = z_steps(3, *rings) + far_parts(most_z[2], 384, 0) + far_parts(few_z[2], 128, 768)
    logs_cut = power([(0, 3), (3, 1)], "late", notes, lists, None, late, sums, second, True)
    logs = jnp.zeros((256, 1024), bf16)
    for place, step in enumerate(POSITIONS):
        piece = logs_cut[place * 256 : place * 256 + 256]
        piece = ring_y(piece, -step) if step else piece
        logs = lax.dynamic_update_slice_in_dim(logs, piece, (y + step) % NY * 256, 1)
    contract = (((0,), (0,)), ((), ()))
    gram = jnp.zeros((128, 1024), jnp.float32)
    for rows in gather_x(logs, 3):
        columns = lax.dynamic_slice_in_dim(rows, rank * 128, 128, 1)
        gram += lax.dot_general(columns, rows, contract, preferred_element_type=jnp.float32)
    return logs, gram / 2048


def solution(mesh):
    placed = (
        P(("grp", "row"), None),
        P(("grp", "row")),
        P(("grp", "row"), None, None),
        P(("grp", "row")),
        P(("grp", "row")),
        P(("grp", "row")),
        P(("grp", "row"), None),
    )

    return jax.shard_map(
        step_body,
        mesh=mesh,
        in_specs=placed,
        out_specs=(P(("grp", "row"), None), P(("grp", "row"), None)),
        check_vma=False,
    )
```
